128 devices in a mesh: part: 1, tp: 2 (over core), dp: 64 (over z, y, x).
Axes of the slice: x: 4, y: 4, z: 4, core: 2. Of those that a mesh axis runs over, the one named last changes fastest.
Arguments:
- hidden: bfloat16 [128, 2048, 768], P(('part', 'dp', 'tp'))
- ln_gain: float32 [768], replicated
- w_in: bfloat16 [768, 7040], P(None, ('dp', 'tp'))
- w_out: bfloat16 [3840, 768], P(('dp', 'tp'))
Outputs:
- output 1: bfloat16 [128, 2048, 768], P(('part', 'dp', 'tp'))
- output 2: bfloat16 [128, 2048, 64], P(('part', 'dp', 'tp'))
- output 3: bfloat16 [128, 2048, 64], P(('part', 'dp', 'tp'))
All inputs are finite; a program needn't handle non-finite values.
Results may differ from the reference program's by a relative error of at most 0.00275064.
Values are sent between devices in bfloat16 or wider.
A program may use at most 1 GiB of HBM per device.

```python
import jax
import jax.numpy as jnp
from jax import lax

D = 768
HEADS = 12
HEAD = 64
BATCH = 128
SEQ = 2048

FF = 4 * D
Q_WIDTH = HEADS * HEAD
JOINT = Q_WIDTH + 2 * HEAD + 2 * FF
MIXED = Q_WIDTH + FF
Q_BLOCK = min(SEQ, 512)
LN_EPS = 1e-6
ROPE_BASE = 10000.0
ATTN_GAIN = 3.0


def setup_inputs(seed: int = 0, part: int = 0) -> dict:
    root_key = jax.random.key(seed)
    key_hidden, key_gain, key_in, key_out = jax.random.split(root_key, 4)
    key_hidden = jax.random.fold_in(key_hidden, part)
    hidden = jax.random.normal(key_hidden, (BATCH, SEQ, D), jnp.float32)
    ln_gain = 1.0 + 0.25 * jax.random.normal(key_gain, (D,), jnp.float32)
    w_in = jax.random.normal(key_in, (D, JOINT), jnp.float32) * D ** -0.5
    row_scale = jnp.where(jnp.arange(MIXED) < Q_WIDTH, ATTN_GAIN, 1.0) * MIXED ** -0.5
    w_out = jax.random.normal(key_out, (MIXED, D), jnp.float32) * row_scale[:, None]
    return {'hidden': hidden.astype(jnp.bfloat16), 'ln_gain': ln_gain,
            'w_in': w_in.astype(jnp.bfloat16), 'w_out': w_out.astype(jnp.bfloat16)}


def rotate(values):
    half_dim = HEAD // 2
    inv_freq = ROPE_BASE ** (-jnp.arange(half_dim, dtype=jnp.float32) * 2.0 / HEAD)
    angles = jnp.arange(SEQ, dtype=jnp.float32)[:, None] * inv_freq[None, :]
    tab_shape = (SEQ,) + (1,) * (values.ndim - 2) + (half_dim,)
    cos_tab = jnp.cos(angles).reshape(tab_shape)
    sin_tab = jnp.sin(angles).reshape(tab_shape)
    first_half = values[..., :half_dim]
    second_half = values[..., half_dim:]
    return jnp.concatenate([first_half * cos_tab - second_half * sin_tab,
                            second_half * cos_tab + first_half * sin_tab], axis=-1)


def attention(q_rot, k_rot, v_seq):
    k_wide = k_rot.astype(jnp.float32)
    v_wide = v_seq.astype(jnp.float32)
    key_pos = jnp.arange(SEQ)
    q_blocks = q_rot.reshape(SEQ // Q_BLOCK, Q_BLOCK, HEADS, HEAD)

    def one_block(item):
        blk_idx, q_tile = item
        scores = jnp.einsum('qhe,ke->qhk', q_tile.astype(jnp.float32), k_wide) * HEAD ** -0.5
        q_pos = blk_idx * Q_BLOCK + jnp.arange(Q_BLOCK)
        allowed = key_pos[None, :] <= q_pos[:, None]
        scores = jnp.where(allowed[:, None, :], scores, -1e30)
        attn_prob = jax.nn.softmax(scores, axis=-1).astype(jnp.bfloat16)
        return jnp.einsum('qhk,ke->qhe', attn_prob.astype(jnp.float32), v_wide).astype(jnp.bfloat16)

    out_tiles = lax.map(one_block, (jnp.arange(SEQ // Q_BLOCK), q_blocks))
    return out_tiles.reshape(SEQ, Q_WIDTH)


def reference(hidden, ln_gain, w_in, w_out):
    def one_request(x_seq):
        x_wide = x_seq.astype(jnp.float32)
        centered = x_wide - jnp.mean(x_wide, axis=-1, keepdims=True)
        row_var = jnp.mean(centered * centered, axis=-1, keepdims=True)
        h_seq = (centered * lax.rsqrt(row_var + LN_EPS) * ln_gain).astype(jnp.bfloat16)
        joint_out = jnp.dot(h_seq, w_in, preferred_element_type=jnp.float32).astype(jnp.bfloat16)
        q_raw = joint_out[:, :Q_WIDTH].reshape(SEQ, HEADS, HEAD)
        k_raw = joint_out[:, Q_WIDTH:Q_WIDTH + HEAD]
        v_seq = joint_out[:, Q_WIDTH + HEAD:Q_WIDTH + 2 * HEAD]
        gate_proj = joint_out[:, Q_WIDTH + 2 * HEAD:Q_WIDTH + 2 * HEAD + FF]
        up_proj = joint_out[:, Q_WIDTH + 2 * HEAD + FF:]
        q_rot = rotate(q_raw.astype(jnp.float32)).astype(jnp.bfloat16)
        k_rot = rotate(k_raw.astype(jnp.float32)).astype(jnp.bfloat16)
        attn_out = attention(q_rot, k_rot, v_seq)
        mlp_out = (jax.nn.silu(gate_proj.astype(jnp.float32)) * up_proj.astype(jnp.float32)).astype(jnp.bfloat16)
        mixed_rows = jnp.concatenate([attn_out, mlp_out], axis=-1)
        proj_out = jnp.dot(mixed_rows, w_out, preferred_element_type=jnp.float32)
        y_seq = (x_wide + proj_out).astype(jnp.bfloat16)
        return (y_seq, k_rot, v_seq)

    y_all, k_all, v_all = lax.map(one_request, hidden)
    return (y_all, k_all, v_all)
```

```python
import functools

import jax
import jax.numpy as jnp
import numpy as np
from jax import lax
from jax.experimental import pallas as pl
from jax.experimental.pallas import tpu as pltpu
from jax.sharding import PartitionSpec as P

LN_EPS = 1e-6
ROPE_BASE = 10000.0
LOG2E = 1.4426950408889634
TILE = 256
FF_CHUNK = 512
ROW_CHUNK = 512
F32 = jnp.float32
BF16 = jnp.bfloat16


def dot_nt(a, b):
    return lax.dot_general(a, b, (((1,), (1,)), ((), ())), preferred_element_type=F32)


def rope_tables(seq_len, head_dim):
    half_dim = head_dim // 2
    inv_freq = ROPE_BASE ** (-np.arange(half_dim, dtype=np.float64) * 2.0 / head_dim)
    angles = inv_freq.astype(np.float32).astype(np.float64)[:, None] * np.arange(seq_len)[None, :]
    angles = angles.astype(np.float32).astype(np.float64)
    return np.cos(angles).astype(np.float32), np.sin(angles).astype(np.float32)


def attention_body(heads, head_dim, x_ref, gain_ref, wq_ref, cos_ref, sin_ref, h_ref, attn_ref, kt_ref, vt_ref,
                   qt, ks, s_a, s_b, ot):
    seq_len, width = x_ref.shape
    q_width = heads * head_dim
    half = head_dim // 2
    n_tiles = seq_len // TILE

    def norm_rows(t, carry):
        rows = pl.ds(pl.multiple_of(t * TILE, TILE), TILE)
        x_wide = x_ref[rows, :].astype(F32)
        centered = x_wide - jnp.mean(x_wide, axis=-1, keepdims=True)
        row_var = jnp.mean(centered * centered, axis=-1, keepdims=True)
        h_ref[rows, :] = (centered * lax.rsqrt(row_var + LN_EPS) * gain_ref[...]).astype(BF16)
        return carry

    lax.fori_loop(0, n_tiles, norm_rows, 0)

    def project(t, carry):
        cols = pl.ds(pl.multiple_of(t * TILE, TILE), TILE)
        pt = dot_nt(wq_ref[...], h_ref[cols, :]).astype(BF16)
        cos_t = cos_ref[:, cols]
        sin_t = sin_ref[:, cols]
        for g in range(heads + 1):
            a = pt[g * head_dim:g * head_dim + half, :].astype(F32)
            b = pt[g * head_dim + half:(g + 1) * head_dim, :].astype(F32)
            rot = jnp.concatenate([a * cos_t - b * sin_t, b * cos_t + a * sin_t], axis=0)
            if g < heads:
                qt[g * head_dim:(g + 1) * head_dim, cols] = rot.astype(BF16)
            else:
                kt_ref[:, cols] = rot.astype(BF16)
                ks[cols, :] = rot.T.astype(BF16)
        vt_ref[:, cols] = pt[q_width + head_dim:q_width + 2 * head_dim, :]
        return carry

    lax.fori_loop(0, n_tiles, project, 0)

    coef = LOG2E * head_dim ** -0.5

    for i in range(n_tiles):
        cols = slice(i * TILE, (i + 1) * TILE)

        def score_tile(h, j, s_ref, m8):
            rows = slice(j * TILE, (j + 1) * TILE)
            hd = pl.ds(pl.multiple_of(h * head_dim, head_dim), head_dim)
            s = jnp.dot(ks[rows, :], qt[hd, cols], preferred_element_type=F32)
            if j == i:
                key = lax.broadcasted_iota(jnp.int32, (TILE, TILE), 0)
                qry = lax.broadcasted_iota(jnp.int32, (TILE, TILE), 1)
                s = jnp.where(key <= qry, s, -1e30)
            s_ref[rows, :] = s
            top = jnp.max(s.reshape(TILE // 8, 8, TILE), axis=0)
            return top if m8 is None else jnp.maximum(m8, top)

        def mix_tile(j, s_ref, m, l8, acc):
            rows = slice(j * TILE, (j + 1) * TILE)
            p = jnp.exp2((s_ref[rows, :] - m) * coef)
            part = jnp.sum(p.reshape(TILE // 8, 8, TILE), axis=0)
            o = jnp.dot(vt_ref[:, rows], p.astype(BF16), preferred_element_type=F32)
            return (part, o) if l8 is None else (l8 + part, acc + o)

        def finish(h, l8, acc):
            hd = pl.ds(pl.multiple_of(h * head_dim, head_dim), head_dim)
            ot[hd, :] = (acc / jnp.sum(l8, axis=0, keepdims=True)).astype(BF16)

        def step(h_mix, s_mix, m_mix, h_next, s_next):
            m8 = l8 = acc = None
            m = jnp.max(m_mix, axis=0, keepdims=True)
            for j in range(i + 1):
                m8 = score_tile(h_next, j, s_next, m8)
                l8, acc = mix_tile(j, s_mix, m, l8, acc)
            finish(h_mix, l8, acc)
            return m8

        m8 = None
        for j in range(i + 1):
            m8 = score_tile(0, j, s_a, m8)

        def pair(t, m8):
            h = 2 * t
            m8_b = step(h, s_a, m8, h + 1, s_b)
            return step(h + 1, s_b, m8_b, jnp.minimum(h + 2, heads - 1), s_a)

        lax.fori_loop(0, heads // 2, pair, m8)
        attn_ref[cols, :] = ot[...].T


def attention_call(x, gain, wq, cos_t, sin_t, heads, head_dim):
    seq_len, width = x.shape
    q_width = heads * head_dim
    vmem = pl.BlockSpec(memory_space=pltpu.VMEM)
    return pl.pallas_call(
        functools.partial(attention_body, heads, head_dim),
        out_shape=(jax.ShapeDtypeStruct((seq_len, width), BF16),
                   jax.ShapeDtypeStruct((seq_len, q_width), BF16),
                   jax.ShapeDtypeStruct((head_dim, seq_len), BF16),
                   jax.ShapeDtypeStruct((head_dim, seq_len), BF16)),
        in_specs=[vmem] * 5,
        out_specs=(vmem,) * 4,
        scratch_shapes=[
            pltpu.VMEM((q_width, seq_len), BF16),
            pltpu.VMEM((seq_len, head_dim), BF16),
            pltpu.VMEM((seq_len, TILE), F32),
            pltpu.VMEM((seq_len, TILE), F32),
            pltpu.VMEM((q_width, TILE), BF16),
        ],
        compiler_params=pltpu.CompilerParams(vmem_limit_bytes=60 * 1024 * 1024),
        name="attention",
    )(x, gain, wq, cos_t, sin_t)


def mlp_body(h_ref, attn_ref, x_ref, wg_ref, wu_ref, wd_ref, wa_ref, y_ref, acc):
    j = pl.program_id(0)
    last = pl.num_programs(0) - 1
    n_rows = h_ref.shape[0] // ROW_CHUNK

    def rows_of(t):
        return pl.ds(t * ROW_CHUNK, ROW_CHUNK)

    @pl.when(j == 0)
    def _():
        for t in range(n_rows):
            r = rows_of(t)
            acc[r, :] = x_ref[r, :].astype(F32) + jnp.dot(attn_ref[r, :], wa_ref[...], preferred_element_type=F32)

    for t in range(n_rows):
        r = rows_of(t)
        gate = dot_nt(h_ref[r, :], wg_ref[...]).astype(BF16).astype(F32)
        up = dot_nt(h_ref[r, :], wu_ref[...]).astype(BF16).astype(F32)
        m = (gate * jax.nn.sigmoid(gate) * up).astype(BF16)
        acc[r, :] += jnp.dot(m, wd_ref[...], preferred_element_type=F32)

    @pl.when(j == last)
    def _():
        y_ref[...] = acc[...].astype(BF16)


def mlp_call(h, attn, x, w_in_t, w_out, gate_at, ff_width):
    seq_len, width = x.shape
    q_width = attn.shape[1]
    whole = pl.BlockSpec((seq_len, width), lambda j: (0, 0))
    n_chunks = ff_width // FF_CHUNK

    def rows_from(start):
        return pl.BlockSpec((pl.Element(FF_CHUNK), pl.Element(width)), lambda j: ((start // 16 + j * (FF_CHUNK // 16)) * 16, 0))

    return pl.pallas_call(
        mlp_body,
        out_shape=jax.ShapeDtypeStruct((seq_len, width), BF16),
        grid=(n_chunks,),
        in_specs=[whole, pl.BlockSpec((seq_len, q_width), lambda j: (0, 0)), whole,
                  rows_from(gate_at), rows_from(gate_at + ff_width), rows_from(q_width),
                  pl.BlockSpec((q_width, width), lambda j: (0, 0))],
        out_specs=whole,
        scratch_shapes=[pltpu.VMEM((seq_len, width), F32)],
        compiler_params=pltpu.CompilerParams(vmem_limit_bytes=60 * 1024 * 1024),
        name="mlp",
    )(h, attn, x, w_in_t, w_in_t, w_out, w_out)


def solution(mesh):
    tok_spec = P(('part', 'dp', 'tp'))

    def per_device(x_blk, ln_gain, w_in_blk, w_out_blk):
        _, seq_len, width = x_blk.shape
        x = x_blk[0]
        w_in_t = lax.all_gather(w_in_blk.T, ('dp', 'tp'), axis=0, tiled=True)
        w_out = lax.all_gather(w_out_blk, ('dp', 'tp'), axis=0, tiled=True)
        ff_width = 4 * width
        q_width = w_out.shape[0] - ff_width
        head_dim = (w_in_t.shape[0] - w_out.shape[0] - ff_width) // 2
        gate_at = q_width + 2 * head_dim
        cos_t, sin_t = rope_tables(seq_len, head_dim)
        h, attn, kt, vt = attention_call(x, ln_gain.reshape(1, width), w_in_t[:gate_at], jnp.asarray(cos_t),
                                         jnp.asarray(sin_t), q_width // head_dim, head_dim)
        y = mlp_call(h, attn, x, w_in_t, w_out, gate_at, ff_width)
        return y[None], kt.T[None], vt.T[None]

    return jax.shard_map(per_device, mesh=mesh,
                         in_specs=(tok_spec, P(), P(None, ('dp', 'tp')), P(('dp', 'tp'), None)),
                         out_specs=(tok_spec, tok_spec, tok_spec), check_vma=False)
```
